32 devices in a mesh: lat: 4 (over y, core), lon: 4 (over z), lev: 2 (over x).
Axes of the slice: x: 2, y: 2, z: 4, core: 2. Of those that a mesh axis runs over, the one named last changes fastest.
Arguments:
- density: float32 [128, 16, 256, 128], P('lat', 'lon', 'lev'), may hold values from 0.2 to 1.8
- crowding: float32 [128, 16, 256, 128], P('lat', 'lon', 'lev'), may hold values from 0.5 to 2
Outputs:
- running_total: float32 [128, 16, 256, 128], P('lat', 'lon', 'lev')
- density_end: float32 [128, 16, 256, 128], P('lat', 'lon', 'lev')
The draws below stay inside these ranges and needn't reach their ends.
All inputs are finite; a program needn't handle non-finite values.
Results may differ from the reference program's by a relative error of at most 0.00002.
Values sent between devices are 32-bit elements; how exact they have to be, the bound alone decides.
A program may use at most 320 MiB of HBM per device.

```python
import jax
import jax.numpy as jnp
from jax import lax

GRID_J = 128
GRID_I = 16
GRID_K = 256
LEVELS = 128
STEPS = 4


def level_of(stream_key, shape, split, smallest, largest):
    level, own = 1.0, jax.random.fold_in(stream_key, 6)
    for dim, shards_of in split:
        heights = jnp.exp(jax.random.uniform(jax.random.fold_in(own, dim), (shards_of,), jnp.float32, smallest / len(split), largest / len(split)))
        level = level * jnp.repeat(heights, shape[dim] // shards_of).reshape([-1 if axis == dim else 1 for axis in range(len(shape))])
    return level


def setup_inputs(seed: int = 0) -> dict:
    key_list = jax.random.split(jax.random.key(seed), 3)
    density = jnp.clip(0.2 + 1.5999999 * jax.random.uniform(key_list[0], (GRID_J, GRID_I, GRID_K, LEVELS), jnp.float32) ** level_of(key_list[0], (GRID_J, GRID_I, GRID_K, LEVELS), ((0, 4), (1, 4), (2, 2)), -0.2, 0.2), 0.2, 1.8)
    crowding = jnp.clip(0.5 + 1.5 * jax.random.uniform(key_list[1], (GRID_J, GRID_I, GRID_K, LEVELS), jnp.float32) ** level_of(key_list[1], (GRID_J, GRID_I, GRID_K, LEVELS), ((0, 4), (1, 4), (2, 2)), -0.2, 0.2), 0.5, 2.0)
    return dict(density=density, crowding=crowding)


def without_rim(values, dims):
    for dim in dims:
        values = lax.slice_in_dim(values, 1, values.shape[dim] - 1, axis=dim)
    return values


def shifted_cells(values, dim, start, dims):
    others = [other for other in dims if other != dim]
    values = without_rim(values, others)
    return lax.slice_in_dim(values, start, start + values.shape[dim] - 2, axis=dim)


def march_step(padded, crowding):
    middle = without_rim(padded, (0, 1, 2))
    lower = [shifted_cells(padded, dim, 0, (0, 1, 2)) for dim in (0, 1, 2)]
    upper = [shifted_cells(padded, dim, 2, (0, 1, 2)) for dim in (0, 1, 2)]
    spread = lower[0] + upper[0] + lower[1] + upper[1] + lower[2] + upper[2] - 6.0 * middle
    return middle + 0.1 * spread + 0.2 * middle * (1.0 - middle * crowding)


def reference(density, crowding):
    for step in range(STEPS):
        density = march_step(jnp.pad(density, ((1, 1), (1, 1), (1, 1), (0, 0)), mode="wrap"), crowding)
    running_total = jnp.cumsum(density, axis=1) / GRID_I
    return running_total, density
```

```python
import functools

import jax
import jax.numpy as jnp
from jax import lax
from jax.experimental import pallas as pl
from jax.experimental.pallas import tpu as pltpu
from jax.sharding import PartitionSpec as P

STEPS = 4
CHUNKS = 16
MESH = pl.DeviceIdType.MESH
LO, HI = 0, 1


def kernel(
    sizes, density, crowding, running, density_end,
    field, crowd, lon, lev,
    load_sem, crowd_sem, store_sem,
    lon_send, lon_recv, lev_send, lev_recv, lat_send, lat_recv, credit,
):
    n_lat, n_lon, n_lev = sizes
    J, I, K, L = density.shape
    rows = max(1, J // CHUNKS)
    chunks = J // rows
    names = {"lat": n_lat, "lon": n_lon, "lev": n_lev}
    me = {name: lax.axis_index(name) for name in names}
    near = {
        name: (
            {name: lax.rem(me[name] + n - 1, n)},
            {name: lax.rem(me[name] + 1, n)},
        )
        for name, n in names.items()
    }

    def load(c):
        own = pl.ds(c * rows, rows)
        return pltpu.make_async_copy(density.at[own], field.at[0, pl.ds(1 + c * rows, rows)], load_sem.at[c])

    def load_crowd(c):
        own = pl.ds(c * rows, rows)
        return pltpu.make_async_copy(crowding.at[own], crowd.at[own], crowd_sem.at[c])

    def store(slot, c, target, which):
        return pltpu.make_async_copy(
            field.at[slot, pl.ds(1 + c * rows, rows)], target.at[pl.ds(c * rows, rows)], store_sem.at[which, c]
        )

    def lon_copy(slot, side, c):
        plane = 0 if side == LO else I - 1
        return pltpu.make_async_remote_copy(
            src_ref=field.at[slot, pl.ds(1 + c * rows, rows), plane],
            dst_ref=lon.at[1 - side, pl.ds(c * rows, rows)],
            send_sem=lon_send.at[side, c],
            recv_sem=lon_recv.at[1 - side, c],
            device_id=near["lon"][side],
            device_id_type=MESH,
        )

    def lev_copy(slot, side, c):
        first = 0 if side == LO else K - 8
        return pltpu.make_async_remote_copy(
            src_ref=field.at[slot, pl.ds(1 + c * rows, rows), :, pl.ds(first, 8)],
            dst_ref=lev.at[slot, 1 - side, pl.ds(c * rows, rows)],
            send_sem=lev_send.at[side, c],
            recv_sem=lev_recv.at[slot, 1 - side, c],
            device_id=near["lev"][side],
            device_id_type=MESH,
        )

    def lat_copy(slot, side):
        return pltpu.make_async_remote_copy(
            src_ref=field.at[slot, 1 if side == LO else J],
            dst_ref=field.at[slot, J + 1 if side == LO else 0],
            send_sem=lat_send.at[side],
            recv_sem=lat_recv.at[slot, 1 - side],
            device_id=near["lat"][side],
            device_id_type=MESH,
        )

    def at_edges(c, act):
        @pl.when(c == 0)
        def _():
            act(LO)

        @pl.when(c == chunks - 1)
        def _():
            act(HI)

    def start_sends(slot, c):
        for side in (LO, HI):
            lon_copy(slot, side, c).start()
            lev_copy(slot, side, c).start()
        at_edges(c, lambda side: lat_copy(slot, side).start())

    def end_sends(slot, c):
        for side in (LO, HI):
            lon_copy(slot, side, c).wait_send()
            lev_copy(slot, side, c).wait_send()
        at_edges(c, lambda side: lat_copy(slot, side).wait_send())

    def end_receives(slot, c):
        for side in (LO, HI):
            lon_copy(slot, side, c).wait_recv()
            lev_copy(slot, side, c).wait_recv()
        at_edges(c, lambda side: lat_copy(slot, 1 - side).wait_recv())

    def give_credit(side, c):
        pl.semaphore_signal(
            credit.at[1 - side, c], inc=1, device_id=near["lon"][side], device_id_type=MESH
        )

    def loop(count, act):
        def lap(c, carry):
            act(c)
            return carry

        lax.fori_loop(0, count, lap, 0)

    def begin(c):
        load(c).start()

    def begin_crowd(c):
        load_crowd(c).start()

    loop(chunks, begin)
    loop(chunks, begin_crowd)

    barrier = pltpu.get_barrier_semaphore()
    for name in names:
        for side in (LO, HI):
            pl.semaphore_signal(barrier, inc=1, device_id=near[name][side], device_id_type=MESH)
    pl.semaphore_wait(barrier, 2 * len(names))

    def first(c):
        load(c).wait()
        start_sends(0, c)

    loop(chunks, first)

    at_k = lax.broadcasted_iota(jnp.int32, (K, L), 0)

    def advance(slot, j):
        for i in range(I):
            middle = field[slot, j + 1, i]
            below = lon[LO, j] if i == 0 else field[slot, j + 1, i - 1]
            above = lon[HI, j] if i == I - 1 else field[slot, j + 1, i + 1]
            before = jnp.where(at_k == 0, lev[slot, LO, j, i, 7:8], pltpu.roll(middle, 1, 0))
            after = jnp.where(at_k == K - 1, lev[slot, HI, j, i, 0:1], pltpu.roll(middle, K - 1, 0))
            around = (field[slot, j, i] + field[slot, j + 2, i]) + (below + above) + (before + after)
            field[1 - slot, j + 1, i] = middle * (0.6 - 0.2 * (middle * crowd[j, i])) + 0.1 * around

    for step in range(STEPS):
        slot = step % 2
        last = step == STEPS - 1

        def march(c):
            if step == 0:
                load_crowd(c).wait()
            end_receives(slot, c)
            loop(rows, lambda r: advance(slot, c * rows + r))
            give_credit(LO, c)
            if not last:
                give_credit(HI, c)
            end_sends(slot, c)
            if last:
                store(1 - slot, c, density_end, 0).start()
            else:
                pl.semaphore_wait(credit.at[LO, c], 1)
                pl.semaphore_wait(credit.at[HI, c], 1)
                start_sends(1 - slot, c)

        loop(chunks, march)

    done, spare = STEPS % 2, 1 - STEPS % 2
    share = 1.0 / (I * n_lon)

    def total(j):
        so_far = jnp.where(me["lon"] > 0, lon[LO, j], 0.0)
        for i in range(I):
            so_far = so_far + field[done, j + 1, i] * share
            field[spare, j + 1, i] = so_far

    def add_up(c):
        @pl.when(me["lon"] > 0)
        def _():
            lon_copy(spare, HI, c).wait_recv()

        loop(rows, lambda r: total(c * rows + r))
        pl.semaphore_wait(credit.at[HI, c], 1)

        @pl.when(me["lon"] < n_lon - 1)
        def _():
            lon_copy(spare, HI, c).start()

        store(spare, c, running, 1).start()

    loop(chunks, add_up)

    def finish(c):
        @pl.when(me["lon"] < n_lon - 1)
        def _():
            lon_copy(spare, HI, c).wait_send()

        store(done, c, density_end, 0).wait()
        store(spare, c, running, 1).wait()

    loop(chunks, finish)


def body(sizes, density, crowding):
    J, I, K, L = density.shape
    chunks = J // max(1, J // CHUNKS)
    shape = jax.ShapeDtypeStruct(density.shape, jnp.float32)
    dma = pltpu.SemaphoreType.DMA
    return pl.pallas_call(
        functools.partial(kernel, sizes),
        out_shape=(shape, shape),
        in_specs=[pl.BlockSpec(memory_space=pl.ANY)] * 2,
        out_specs=(pl.BlockSpec(memory_space=pl.ANY),) * 2,
        scratch_shapes=[
            pltpu.VMEM((2, J + 2, I, K, L), jnp.float32),
            pltpu.VMEM((J, I, K, L), jnp.float32),
            pltpu.VMEM((2, J, K, L), jnp.float32),
            pltpu.VMEM((2, 2, J, I, 8, L), jnp.float32),
            dma((chunks,)),
            dma((chunks,)),
            dma((2, chunks)),
            dma((2, chunks)),
            dma((2, chunks)),
            dma((2, chunks)),
            dma((2, 2, chunks)),
            dma((2,)),
            dma((2, 2)),
            pltpu.SemaphoreType.REGULAR((2, chunks)),
        ],
        compiler_params=pltpu.CompilerParams(
            collective_id=0, has_side_effects=True, vmem_limit_bytes=67043328
        ),
    )(density, crowding)


def solution(mesh):
    sizes = tuple(mesh.shape[name] for name in ("lat", "lon", "lev"))
    return jax.shard_map(
        functools.partial(body, sizes),
        mesh=mesh,
        in_specs=(P("lat", "lon", "lev", None), P("lat", "lon", "lev", None)),
        out_specs=(P("lat", "lon", "lev", None), P("lat", "lon", "lev", None)),
        check_vma=False,
    )
```

```python
import functools

import jax
import jax.numpy as jnp
from jax import lax
from jax.experimental import pallas as pl
from jax.experimental.pallas import tpu as pltpu
from jax.sharding import PartitionSpec as P

STEPS = 4
CHUNKS = 32
LAG = 2
MESH = pl.DeviceIdType.MESH
LO, HI = 0, 1


def kernel(
    sizes, density, crowding, running, density_end,
    field, crowd, lon, lev,
    load_sem, crowd_sem, store_sem,
    lon_send, lon_recv, lev_send, lev_recv, lat_send, lat_recv, credit,
):
    n_lat, n_lon, n_lev = sizes
    J, I, K, L = density.shape
    rows = max(1, J // CHUNKS)
    chunks = J // rows
    names = {"lat": n_lat, "lon": n_lon, "lev": n_lev}
    me = {name: lax.axis_index(name) for name in names}
    near = {
        name: (
            {name: lax.rem(me[name] + n - 1, n)},
            {name: lax.rem(me[name] + 1, n)},
        )
        for name, n in names.items()
    }

    def load(c):
        own = pl.ds(c * rows, rows)
        return pltpu.make_async_copy(density.at[own], field.at[0, pl.ds(1 + c * rows, rows)], load_sem.at[c])

    def load_crowd(c):
        own = pl.ds(c * rows, rows)
        return pltpu.make_async_copy(crowding.at[own], crowd.at[own], crowd_sem.at[c])

    def store(slot, c, target, which):
        return pltpu.make_async_copy(
            field.at[slot, pl.ds(1 + c * rows, rows)], target.at[pl.ds(c * rows, rows)], store_sem.at[which, c]
        )

    def lon_copy(slot, side, c):
        plane = 0 if side == LO else I - 1
        return pltpu.make_async_remote_copy(
            src_ref=field.at[slot, pl.ds(1 + c * rows, rows), plane],
            dst_ref=lon.at[1 - side, pl.ds(c * rows, rows)],
            send_sem=lon_send.at[side, c],
            recv_sem=lon_recv.at[1 - side, c],
            device_id=near["lon"][side],
            device_id_type=MESH,
        )

    def lev_copy(slot, side, c):
        first = 0 if side == LO else K - 8
        return pltpu.make_async_remote_copy(
            src_ref=field.at[slot, pl.ds(1 + c * rows, rows), :, pl.ds(first, 8)],
            dst_ref=lev.at[slot, 1 - side, pl.ds(c * rows, rows)],
            send_sem=lev_send.at[side, c],
            recv_sem=lev_recv.at[slot, 1 - side, c],
            device_id=near["lev"][side],
            device_id_type=MESH,
        )

    def lat_copy(slot, side):
        return pltpu.make_async_remote_copy(
            src_ref=field.at[slot, 1 if side == LO else J],
            dst_ref=field.at[slot, J + 1 if side == LO else 0],
            send_sem=lat_send.at[side],
            recv_sem=lat_recv.at[slot, 1 - side],
            device_id=near["lat"][side],
            device_id_type=MESH,
        )

    def at_edges(c, act):
        @pl.when(c == 0)
        def _():
            act(LO)

        @pl.when(c == chunks - 1)
        def _():
            act(HI)

    def start_sends(slot, c):
        for side in (LO, HI):
            lon_copy(slot, side, c).start()
            lev_copy(slot, side, c).start()
        at_edges(c, lambda side: lat_copy(slot, side).start())

    def end_sends(slot, c):
        for side in (LO, HI):
            lon_copy(slot, side, c).wait_send()
            lev_copy(slot, side, c).wait_send()
        at_edges(c, lambda side: lat_copy(slot, side).wait_send())

    def end_receives(slot, c):
        for side in (LO, HI):
            lon_copy(slot, side, c).wait_recv()
            lev_copy(slot, side, c).wait_recv()
        at_edges(c, lambda side: lat_copy(slot, 1 - side).wait_recv())

    def give_credit(side, c):
        pl.semaphore_signal(
            credit.at[1 - side, c], inc=1, device_id=near["lon"][side], device_id_type=MESH
        )

    def loop(count, act):
        def lap(c, carry):
            act(c)
            return carry

        lax.fori_loop(0, count, lap, 0)

    def begin(c):
        load(c).start()

    def begin_crowd(c):
        load_crowd(c).start()

    barrier = pltpu.get_barrier_semaphore()
    for name in names:
        for side in (LO, HI):
            pl.semaphore_signal(barrier, inc=1, device_id=near[name][side], device_id_type=MESH)
    loop(chunks, begin)
    pl.semaphore_wait(barrier, 2 * len(names))

    def first(c):
        load(c).wait()
        start_sends(0, c)

    loop(chunks, first)
    loop(chunks, begin_crowd)

    at_k = lax.broadcasted_iota(jnp.int32, (K, L), 0)

    def advance(slot, j):
        for i in range(I):
            middle = field[slot, j + 1, i]
            below = lon[LO, j] if i == 0 else field[slot, j + 1, i - 1]
            above = lon[HI, j] if i == I - 1 else field[slot, j + 1, i + 1]
            before = jnp.where(at_k == 0, lev[slot, LO, j, i, 7:8], pltpu.roll(middle, 1, 0))
            after = jnp.where(at_k == K - 1, lev[slot, HI, j, i, 0:1], pltpu.roll(middle, K - 1, 0))
            around = (field[slot, j, i] + field[slot, j + 2, i]) + (below + above) + (before + after)
            field[1 - slot, j + 1, i] = middle * (0.6 - 0.2 * (middle * crowd[j, i])) + 0.1 * around

    done, spare = STEPS % 2, 1 - STEPS % 2
    lag = min(LAG, chunks)
    share = 1.0 / (I * n_lon)

    def total(j):
        so_far = jnp.where(me["lon"] > 0, lon[LO, j], 0.0)
        for i in range(I):
            so_far = so_far + field[done, j + 1, i] * share
            field[spare, j + 1, i] = so_far

    def add_up(c):
        @pl.when(me["lon"] > 0)
        def _():
            lon_copy(spare, HI, c).wait_recv()

        loop(rows, lambda r: total(c * rows + r))
        pl.semaphore_wait(credit.at[HI, c], 1)

        @pl.when(me["lon"] < n_lon - 1)
        def _():
            lon_copy(spare, HI, c).start()

        store(spare, c, running, 1).start()

    for step in range(STEPS):
        slot = step % 2
        last = step == STEPS - 1

        def march(c):
            if step == 0:
                load_crowd(c).wait()
            end_receives(slot, c)
            loop(rows, lambda r: advance(slot, c * rows + r))
            give_credit(LO, c)
            if not last:
                give_credit(HI, c)
            end_sends(slot, c)
            if last:
                store(1 - slot, c, density_end, 0).start()

                @pl.when(c >= lag)
                def _():
                    add_up(c - lag)
            else:
                pl.semaphore_wait(credit.at[LO, c], 1)
                pl.semaphore_wait(credit.at[HI, c], 1)
                start_sends(1 - slot, c)

        loop(chunks, march)

    loop(lag, lambda c: add_up(chunks - lag + c))

    def finish(c):
        @pl.when(me["lon"] < n_lon - 1)
        def _():
            lon_copy(spare, HI, c).wait_send()

        store(done, c, density_end, 0).wait()
        store(spare, c, running, 1).wait()

    loop(chunks, finish)


def body(sizes, density, crowding):
    J, I, K, L = density.shape
    chunks = J // max(1, J // CHUNKS)
    shape = jax.ShapeDtypeStruct(density.shape, jnp.float32)
    dma = pltpu.SemaphoreType.DMA
    return pl.pallas_call(
        functools.partial(kernel, sizes),
        out_shape=(shape, shape),
        in_specs=[pl.BlockSpec(memory_space=pl.ANY)] * 2,
        out_specs=(pl.BlockSpec(memory_space=pl.ANY),) * 2,
        scratch_shapes=[
            pltpu.VMEM((2, J + 2, I, K, L), jnp.float32),
            pltpu.VMEM((J, I, K, L), jnp.float32),
            pltpu.VMEM((2, J, K, L), jnp.float32),
            pltpu.VMEM((2, 2, J, I, 8, L), jnp.float32),
            dma((chunks,)),
            dma((chunks,)),
            dma((2, chunks)),
            dma((2, chunks)),
            dma((2, chunks)),
            dma((2, chunks)),
            dma((2, 2, chunks)),
            dma((2,)),
            dma((2, 2)),
            pltpu.SemaphoreType.REGULAR((2, chunks)),
        ],
        compiler_params=pltpu.CompilerParams(
            collective_id=0, has_side_effects=True, vmem_limit_bytes=67043328
        ),
    )(density, crowding)


def solution(mesh):
    sizes = tuple(mesh.shape[name] for name in ("lat", "lon", "lev"))
    return jax.shard_map(
        functools.partial(body, sizes),
        mesh=mesh,
        in_specs=(P("lat", "lon", "lev", None), P("lat", "lon", "lev", None)),
        out_specs=(P("lat", "lon", "lev", None), P("lat", "lon", "lev", None)),
        check_vma=False,
    )
```

```python
import functools

import jax
import jax.numpy as jnp
from jax import lax
from jax.experimental import pallas as pl
from jax.experimental.pallas import tpu as pltpu
from jax.sharding import PartitionSpec as P

STEPS = 4
CHUNKS = 16
MESH = pl.DeviceIdType.MESH
LO, HI = 0, 1


def kernel(
    sizes, density, crowding, running, density_end,
    field, crowd, lon, lev,
    load_sem, crowd_sem,
    lon_send, lon_recv, lev_send, lev_recv, lat_send, lat_recv, credit,
):
    n_lat, n_lon, n_lev = sizes
    J, I, K, L = density.shape
    rows = max(1, J // CHUNKS)
    chunks = J // rows
    names = {"lat": n_lat, "lon": n_lon, "lev": n_lev}
    me = {name: lax.axis_index(name) for name in names}
    near = {
        name: (
            {name: lax.rem(me[name] + n - 1, n)},
            {name: lax.rem(me[name] + 1, n)},
        )
        for name, n in names.items()
    }

    def load(c):
        own = pl.ds(c * rows, rows)
        return pltpu.make_async_copy(density.at[own], field.at[0, pl.ds(1 + c * rows, rows)], load_sem.at[c])

    def load_crowd(c):
        own = pl.ds(c * rows, rows)
        return pltpu.make_async_copy(crowding.at[own], crowd.at[own], crowd_sem.at[c])

    def lon_copy(slot, side, c):
        plane = 0 if side == LO else I - 1
        return pltpu.make_async_remote_copy(
            src_ref=field.at[slot, pl.ds(1 + c * rows, rows), plane],
            dst_ref=lon.at[1 - side, pl.ds(c * rows, rows)],
            send_sem=lon_send.at[side, c],
            recv_sem=lon_recv.at[1 - side, c],
            device_id=near["lon"][side],
            device_id_type=MESH,
        )

    def total_copy(c):
        own = pl.ds(c * rows, rows)
        return pltpu.make_async_remote_copy(
            src_ref=running.at[own, I - 1],
            dst_ref=lon.at[LO, own],
            send_sem=lon_send.at[HI, c],
            recv_sem=lon_recv.at[LO, c],
            device_id=near["lon"][HI],
            device_id_type=MESH,
        )

    def lev_copy(slot, side, c):
        first = 0 if side == LO else K - 8
        return pltpu.make_async_remote_copy(
            src_ref=field.at[slot, pl.ds(1 + c * rows, rows), :, pl.ds(first, 8)],
            dst_ref=lev.at[slot, 1 - side, pl.ds(c * rows, rows)],
            send_sem=lev_send.at[side, c],
            recv_sem=lev_recv.at[slot, 1 - side, c],
            device_id=near["lev"][side],
            device_id_type=MESH,
        )

    def lat_copy(slot, side):
        return pltpu.make_async_remote_copy(
            src_ref=field.at[slot, 1 if side == LO else J],
            dst_ref=field.at[slot, J + 1 if side == LO else 0],
            send_sem=lat_send.at[side],
            recv_sem=lat_recv.at[slot, 1 - side],
            device_id=near["lat"][side],
            device_id_type=MESH,
        )

    def at_edges(c, act):
        @pl.when(c == 0)
        def _():
            act(LO)

        @pl.when(c == chunks - 1)
        def _():
            act(HI)

    def start_sends(slot, c):
        for side in (LO, HI):
            lon_copy(slot, side, c).start()
            lev_copy(slot, side, c).start()
        at_edges(c, lambda side: lat_copy(slot, side).start())

    def end_sends(slot, c):
        for side in (LO, HI):
            lon_copy(slot, side, c).wait_send()
            lev_copy(slot, side, c).wait_send()
        at_edges(c, lambda side: lat_copy(slot, side).wait_send())

    def end_receives(slot, c):
        for side in (LO, HI):
            lon_copy(slot, side, c).wait_recv()
            lev_copy(slot, side, c).wait_recv()
        at_edges(c, lambda side: lat_copy(slot, 1 - side).wait_recv())

    def give_credit(side, c):
        pl.semaphore_signal(
            credit.at[1 - side, c], inc=1, device_id=near["lon"][side], device_id_type=MESH
        )

    def loop(count, act):
        def lap(c, carry):
            act(c)
            return carry

        lax.fori_loop(0, count, lap, 0)

    def begin(c):
        load(c).start()

    def begin_crowd(c):
        load_crowd(c).start()

    barrier = pltpu.get_barrier_semaphore()
    for name in names:
        for side in (LO, HI):
            pl.semaphore_signal(barrier, inc=1, device_id=near[name][side], device_id_type=MESH)
    loop(chunks, begin)
    pl.semaphore_wait(barrier, 2 * len(names))

    def first(c):
        load(c).wait()
        start_sends(0, c)

    loop(chunks, first)
    loop(chunks, begin_crowd)

    at_k = lax.broadcasted_iota(jnp.int32, (K, L), 0)

    def advance(slot, j, put):
        for i in range(I):
            middle = field[slot, j + 1, i]
            below = lon[LO, j] if i == 0 else field[slot, j + 1, i - 1]
            above = lon[HI, j] if i == I - 1 else field[slot, j + 1, i + 1]
            before = jnp.where(at_k == 0, lev[slot, LO, j, i, 7:8], pltpu.roll(middle, 1, 0))
            after = jnp.where(at_k == K - 1, lev[slot, HI, j, i, 0:1], pltpu.roll(middle, K - 1, 0))
            around = (field[slot, j, i] + field[slot, j + 2, i]) + (below + above) + (before + after)
            put(j, i, middle * (0.6 - 0.2 * (middle * crowd[j, i])) + 0.1 * around)

    share = 1.0 / (I * n_lon)

    def total(j):
        so_far = jnp.where(me["lon"] > 0, lon[LO, j], 0.0)
        for i in range(I):
            so_far = so_far + density_end[j, i] * share
            running[j, i] = so_far

    def add_up(c):
        @pl.when(me["lon"] > 0)
        def _():
            total_copy(c).wait_recv()

        loop(rows, lambda r: total(c * rows + r))
        pl.semaphore_wait(credit.at[HI, c], 1)

        @pl.when(me["lon"] < n_lon - 1)
        def _():
            total_copy(c).start()

    for step in range(STEPS):
        slot = step % 2
        last = step == STEPS - 1

        def put(j, i, value):
            if last:
                density_end[j, i] = value
            else:
                field[1 - slot, j + 1, i] = value

        def march(c):
            if step == 0:
                load_crowd(c).wait()
            end_receives(slot, c)
            loop(rows, lambda r: advance(slot, c * rows + r, put))
            give_credit(LO, c)
            if not last:
                give_credit(HI, c)
            end_sends(slot, c)
            if not last:
                pl.semaphore_wait(credit.at[LO, c], 1)
                pl.semaphore_wait(credit.at[HI, c], 1)
                start_sends(1 - slot, c)

        loop(chunks, march)

    loop(chunks, add_up)

    def finish(c):
        @pl.when(me["lon"] < n_lon - 1)
        def _():
            total_copy(c).wait_send()

    loop(chunks, finish)


def body(sizes, density, crowding):
    J, I, K, L = density.shape
    chunks = J // max(1, J // CHUNKS)
    shape = pltpu.VMEM(density.shape, jnp.float32)
    dma = pltpu.SemaphoreType.DMA
    return pl.pallas_call(
        functools.partial(kernel, sizes),
        out_shape=(shape, shape),
        in_specs=[pl.BlockSpec(memory_space=pl.ANY)] * 2,
        out_specs=(pl.BlockSpec(memory_space=pltpu.VMEM),) * 2,
        scratch_shapes=[
            pltpu.VMEM((2, J + 2, I, K, L), jnp.float32),
            pltpu.VMEM((J, I, K, L), jnp.float32),
            pltpu.VMEM((2, J, K, L), jnp.float32),
            pltpu.VMEM((2, 2, J, I, 8, L), jnp.float32),
            dma((chunks,)),
            dma((chunks,)),
            dma((2, chunks)),
            dma((2, chunks)),
            dma((2, chunks)),
            dma((2, 2, chunks)),
            dma((2,)),
            dma((2, 2)),
            pltpu.SemaphoreType.REGULAR((2, chunks)),
        ],
        compiler_params=pltpu.CompilerParams(
            collective_id=0, has_side_effects=True, vmem_limit_bytes=40 * 2**20
        ),
    )(density, crowding)


def solution(mesh):
    sizes = tuple(mesh.shape[name] for name in ("lat", "lon", "lev"))
    return jax.shard_map(
        functools.partial(body, sizes),
        mesh=mesh,
        in_specs=(P("lat", "lon", "lev", None), P("lat", "lon", "lev", None)),
        out_specs=(P("lat", "lon", "lev", None), P("lat", "lon", "lev", None)),
        check_vma=False,
    )
```
